32 devices in a mesh: seq: 8 (over z, x), batch: 4 (over y, core).
Axes of the slice: x: 2, y: 2, z: 4, core: 2. Of those that a mesh axis runs over, the one named last changes fastest.
Arguments:
- tokens: bfloat16 [4, 2048, 256], P('batch', 'seq'), may hold values from -6 to 6
- out_grad: bfloat16 [4, 2048, 256], P('batch', 'seq'), may hold values from -6 to 6
- in_weight: bfloat16 [256, 768], replicated, may hold values from -0.375 to 0.375
- out_weight: bfloat16 [256, 256], replicated, may hold values from -0.375 to 0.375
- skip_bias: float32 [256], replicated, may hold values from -4 to 4
- embed_weight: float32 [5, 64], replicated, may hold values from -4 to 4
- embed_bias: float32 [64], replicated, may hold values from -4 to 4
- hidden_weight: float32 [64, 64], replicated, may hold values from -0.75 to 0.75
- hidden_bias: float32 [64], replicated, may hold values from -4 to 4
- filter_weight: float32 [64, 256], replicated, may hold values from -0.75 to 0.75
- sine_freq: float32 [2, 64], replicated, may hold values from 0.5 to 3
- decay_rate: float32 [256], replicated, may hold values from 0.0014990234 to 0.0074951174
Outputs:
- grad_tokens: bfloat16 [4, 2048, 256], P('batch', 'seq')
- grad_in_weight: float32 [256, 768], replicated
- grad_out_weight: float32 [256, 256], replicated
- grad_skip_bias: float32 [256], replicated
- grad_embed_weight: float32 [5, 64], replicated
- grad_embed_bias: float32 [64], replicated
- grad_hidden_weight: float32 [64, 64], replicated
- grad_hidden_bias: float32 [64], replicated
- grad_filter_weight: float32 [64, 256], replicated
- grad_sine_freq: float32 [2, 64], replicated
The draws below stay inside these ranges and needn't reach their ends.
All inputs are finite; a program needn't handle non-finite values.
Results may differ from the reference program's by a relative error of at most 0.013.
Values may be sent and summed in bfloat16 or wider, within the bound.
A program may use at most 64 MiB of HBM per device.

```python
import math
import jax
import jax.numpy as jnp
from jax import lax

D = 256
HID = 64
EMB = 5
BATCH = 4
LEN = 2048


def block_scale(own_key, dims, pieces, least, high):
    def one(dim, parts):
        heights = jax.random.uniform(jax.random.fold_in(jax.random.fold_in(own_key, 6), dim), (parts,), jnp.float32, least / len(pieces), high / len(pieces))
        return jnp.repeat(jnp.exp(heights), dims[dim] // parts).reshape((-1,) + (1,) * (len(dims) - dim - 1))

    gain = one(*pieces[0])
    for cut in pieces[1:]:
        gain = gain * one(*cut)
    return gain


def gaussian(key, dims, spread, reach, shards=(), kind=jnp.bfloat16):
    entries = jax.random.normal(key, dims, jnp.float32) * spread
    if len(shards) > 0:
        entries = block_scale(key, dims, shards, -0.22, 0.18) * entries
    return jnp.clip(entries, min=-reach, max=reach).astype(kind)


def setup_inputs(seed: int = 0) -> dict:
    splits = jax.random.split(jax.random.key(seed), 13)
    return {
        "tokens": gaussian(splits[0], (BATCH, LEN, D), 1.0, 6.0, ((0, 4), (1, 8))),
        "out_grad": gaussian(splits[1], (BATCH, LEN, D), 1.0, 6.0, ((0, 4), (1, 8))),
        "in_weight": gaussian(splits[2], (D, 3 * D), D ** -0.5, 0.375),
        "out_weight": gaussian(splits[3], (D, D), D ** -0.5, 0.375),
        "skip_bias": gaussian(splits[4], (D,), 1.0, 4.0, (), jnp.float32),
        "embed_weight": gaussian(splits[5], (EMB, HID), 1.0, 4.0, (), jnp.float32),
        "embed_bias": gaussian(splits[6], (HID,), 1.0, 4.0, (), jnp.float32),
        "hidden_weight": gaussian(splits[7], (HID, HID), HID ** -0.5, 0.75, (), jnp.float32),
        "hidden_bias": gaussian(splits[8], (HID,), 1.0, 4.0, (), jnp.float32),
        "filter_weight": gaussian(splits[9], (HID, D), HID ** -0.5, 0.75, (), jnp.float32),
        "sine_freq": jnp.clip(jax.random.uniform(splits[10], (2, HID), jnp.float32, 0.5, 3.0), 0.5, 3.0),
        "decay_rate": jnp.clip(jnp.exp(jax.random.uniform(splits[11], (D,), jnp.float32, math.log(0.0014990234), math.log(0.0074951174))), 0.0014990234, 0.0074951174),
    }


highest = lax.Precision.HIGHEST

def embedding(positions, length, band_count):
    scaled = positions / length
    rows_list = [scaled]
    for band_index in range(1, band_count + 1):
        angle = 2.0 * math.pi * band_index * scaled
        rows_list.append(jnp.cos(angle))
        rows_list.append(jnp.sin(angle))
    return jnp.stack(rows_list, axis=1)

def reference(tokens, out_grad, in_weight, out_weight, skip_bias, embed_weight, embed_bias, hidden_weight, hidden_bias, filter_weight, sine_freq, decay_rate):
    positions = jnp.arange(LEN, dtype=jnp.float32)
    band_count = (EMB - 1) // 2
    embed_rows = embedding(positions, LEN, band_count)
    modul = 4.0 * jnp.exp(-decay_rate[None, :] * positions[:, None]) / math.sqrt(LEN)

    def filter_net(weight_one, bias_one, weight_two, bias_two, weight_three, freqs):
        pre_one = jnp.dot(embed_rows, weight_one, precision=highest) + bias_one
        act_one = jnp.sin(freqs[0] * pre_one)
        pre_two = jnp.dot(act_one, weight_two, precision=highest) + bias_two
        act_two = jnp.sin(freqs[1] * pre_two)
        return jnp.dot(act_two, weight_three, precision=highest) * modul
    filt, pullback = jax.vjp(filter_net, embed_weight, embed_bias, hidden_weight, hidden_bias, filter_weight, sine_freq)
    total = 2 * LEN
    filt_spec = jnp.fft.rfft(filt, n=total, axis=0)

    def one_sequence(inputs):
        tokens_one, grads_one = inputs
        projected = jnp.dot(tokens_one, in_weight, preferred_element_type=jnp.float32)
        gate_out = projected[:, :D].astype(jnp.bfloat16)
        gate_in = projected[:, D:2 * D].astype(jnp.bfloat16)
        values_in = projected[:, 2 * D:].astype(jnp.bfloat16)
        mixed = (values_in.astype(jnp.float32) * gate_in.astype(jnp.float32)).astype(jnp.bfloat16)
        grad_gated = jnp.dot(grads_one, out_weight.T, preferred_element_type=jnp.float32).astype(jnp.bfloat16)
        grad_conv = (grad_gated.astype(jnp.float32) * gate_out.astype(jnp.float32)).astype(jnp.bfloat16)
        mixed_float = mixed.astype(jnp.float32)
        grad_float = grad_conv.astype(jnp.float32)
        mixed_spec = jnp.fft.rfft(mixed_float, n=total, axis=0)
        grad_spec = jnp.fft.rfft(grad_float, n=total, axis=0)
        conv = jnp.fft.irfft(mixed_spec * filt_spec, n=total, axis=0)[:LEN]
        conv = (conv + skip_bias[None, :] * mixed_float).astype(jnp.bfloat16)
        grad_mixed = jnp.fft.irfft(grad_spec * jnp.conj(filt_spec), n=total, axis=0)[:LEN]
        grad_mixed = (grad_mixed + skip_bias[None, :] * grad_float).astype(jnp.bfloat16)
        grad_filt = jnp.fft.irfft(grad_spec * jnp.conj(mixed_spec), n=total, axis=0)[:LEN]
        conv_float = conv.astype(jnp.float32)
        gated = (gate_out.astype(jnp.float32) * conv_float).astype(jnp.bfloat16)
        grad_out_w = jnp.dot(gated.T, grads_one, preferred_element_type=jnp.float32)
        grad_gate_out = (grad_gated.astype(jnp.float32) * conv_float).astype(jnp.bfloat16)
        grad_gate_in = (grad_mixed.astype(jnp.float32) * values_in.astype(jnp.float32)).astype(jnp.bfloat16)
        grad_values = (grad_mixed.astype(jnp.float32) * gate_in.astype(jnp.float32)).astype(jnp.bfloat16)
        grad_proj = jnp.concatenate([grad_gate_out, grad_gate_in, grad_values], axis=1)
        grad_tok = jnp.dot(grad_proj, in_weight.T, preferred_element_type=jnp.float32).astype(jnp.bfloat16)
        grad_in_w = jnp.dot(tokens_one.T, grad_proj, preferred_element_type=jnp.float32)
        grad_bias = lax.optimization_barrier(jnp.sum(grad_float * mixed_float, axis=0))
        return (grad_tok, grad_in_w, grad_out_w, grad_bias, grad_filt)
    results = lax.map(one_sequence, (tokens, out_grad))
    grad_scale = 1.0 / math.sqrt(BATCH * LEN)
    filter_scale = grad_scale / 4.0
    grad_filt_total = lax.optimization_barrier(jnp.sum(results[4], axis=0))
    filter_grads = pullback(grad_filt_total)
    return (results[0], lax.optimization_barrier(jnp.sum(results[1], axis=0)) * grad_scale, lax.optimization_barrier(jnp.sum(results[2], axis=0)) * grad_scale, lax.optimization_barrier(jnp.sum(results[3], axis=0)) * grad_scale, filter_grads[0] * filter_scale, filter_grads[1] * filter_scale, filter_grads[2] * filter_scale, filter_grads[3] * filter_scale, filter_grads[4] * filter_scale, filter_grads[5] * filter_scale)
```

```python
import functools
import math

import jax
import jax.numpy as jnp
import numpy as np
from jax import lax
from jax.experimental import pallas as pl
from jax.experimental.pallas import tpu as pltpu
from jax.sharding import PartitionSpec as P

highest = lax.Precision.HIGHEST
MESH = pl.DeviceIdType.MESH
LANES = 128


def factor(length):
    total = 2 * length
    first_len = 2
    while first_len * first_len < total and total % (2 * first_len) == 0:
        first_len = first_len * 2
    return first_len, total // first_len


def make_tables(length):
    total = 2 * length
    first_len, second_len = factor(length)
    half = first_len // 2
    kept = half + 1
    pad = -(-kept // 8) * 8
    k1 = np.arange(kept)[None, :, None]
    n1 = np.arange(half)[None, None, :]
    n2 = np.arange(second_len)[:, None, None]
    angle = 2.0 * np.pi * ((k1 * (n1 * second_len + n2)) % total) / total
    fwd = np.zeros((second_len, 2 * pad, half), np.float32)
    fwd[:, :kept] = np.cos(angle)
    fwd[:, pad : pad + kept] = -np.sin(angle)
    weight = np.where((k1 == 0) | (k1 == half), 1.0, 2.0) / total
    inv = np.zeros((second_len, half, 2 * pad), np.float32)
    inv[:, :, :kept] = np.swapaxes(weight * np.cos(angle), 1, 2)
    inv[:, :, pad : pad + kept] = np.swapaxes(-weight * np.sin(angle), 1, 2)
    index = np.arange(second_len)
    small = 2.0 * np.pi * ((index[:, None] * index[None, :]) % second_len) / second_len
    cos, sin = np.cos(small), np.sin(small)
    inner = np.block([[cos, sin], [-sin, cos]])
    outer = np.block([[cos, -sin], [sin, cos]])
    return tuple(jnp.asarray(t, jnp.bfloat16) for t in (fwd, inv, inner, outer))


def lane_roll(value, shift):
    shift = shift % LANES
    return value if shift == 0 else pltpu.roll(value, shift, 1)


def conv_kernel(
    axis_n,
    chan,
    scale,
    tok,
    og,
    inw,
    outw,
    filt,
    skip,
    fwd,
    inv,
    inner,
    outer,
    gt_out,
    pk_out,
    y_out,
    bias_out,
    send_one,
    recv_one,
    send_two,
    recv_two,
    gates,
    x_buf,
    z_buf,
    v_buf,
    conv_buf,
    sems,
):
    n = axis_n
    me = lax.axis_index("seq")
    pos, width = tok.shape
    rows = send_one.shape[1]
    fold = pos // rows
    step = 2 * chan
    second_len, double_pad, half = fwd.shape
    pad = double_pad // 2
    kept = half + 1
    f32, bf16 = jnp.float32, jnp.bfloat16

    barrier = pltpu.get_barrier_semaphore()
    for k in range(1, n):
        pl.semaphore_signal(
            barrier, inc=1, device_id={"seq": lax.rem(me + k, n)}, device_id_type=MESH
        )

    proj = jnp.dot(tok[...], inw[...], preferred_element_type=f32)
    gate_out = proj[:, :width].astype(bf16)
    gate_in = proj[:, width : 2 * width].astype(bf16)
    values = proj[:, 2 * width :].astype(bf16)
    gated_grad = lax.dot_general(
        og[...], outw[...], (((1,), (1,)), ((), ())), preferred_element_type=f32
    ).astype(bf16)
    gates[0] = gate_out
    gates[1] = gate_in
    gates[2] = values
    gates[3] = gated_grad
    mixed = (values.astype(f32) * gate_in.astype(f32)).astype(bf16).astype(f32)
    grad = (gated_grad.astype(f32) * gate_out.astype(f32)).astype(bf16).astype(f32)
    bias_out[...] = jnp.sum(mixed * grad, axis=0, keepdims=True)

    lane = lax.broadcasted_iota(jnp.int32, (rows, LANES), 1)
    lane_full = lax.broadcasted_iota(jnp.int32, (pos, LANES), 1)
    for d in range(n):
        tile, off = (d * chan) // LANES * LANES, (d * chan) % LANES
        both = jnp.where(
            lane_full < chan,
            lane_roll(mixed[:, tile : tile + LANES], -off),
            lane_roll(grad[:, tile : tile + LANES], chan - off),
        )
        packed = both[:rows]
        for j in range(1, fold):
            packed = jnp.where(
                lane >= j * step, lane_roll(both[j * rows : (j + 1) * rows], j * step), packed
            )
        send_one[d] = packed.astype(bf16)

    pl.semaphore_wait(barrier, n - 1)

    def copy(send, recv, which, k):
        dest = lax.rem(me + k, n)
        return pltpu.make_async_remote_copy(
            src_ref=send.at[dest],
            dst_ref=recv.at[me],
            send_sem=sems.at[2 * which, k],
            recv_sem=sems.at[2 * which + 1, k],
            device_id={"seq": dest},
            device_id_type=MESH,
        )

    for k in range(1, n):
        copy(send_one, recv_one, 0, k).start()
    recv_one[me] = send_one[me]
    v_buf[...] = jnp.zeros_like(v_buf)
    for k in range(1, n):
        copy(send_one, recv_one, 0, k).wait()

    for s in range(n):
        block = recv_one[s].astype(f32)
        for j in range(fold):
            at = pl.ds(s * pos + j * rows, rows)
            x_buf[at, :] = jnp.where(lane < step, lane_roll(block, -j * step), filt[at, :])

    def stage_one(n2, _):
        part = x_buf[pl.ds(n2, half, stride=second_len), :].astype(bf16)
        z_buf[pl.ds(pl.multiple_of(n2 * double_pad, 8), double_pad), :] = jnp.dot(
            fwd[n2], part, preferred_element_type=f32
        )
        return 0

    lax.fori_loop(0, second_len, stage_one, 0, unroll=8)

    lane_k = lax.broadcasted_iota(jnp.int32, (second_len, LANES), 1)
    low = lane_k < step
    mid = (lane_k >= chan) & (lane_k < step)
    sign = jnp.where((lane_k >= chan), -1.0, 1.0).astype(f32)

    def stage_two(k1, _):
        stacked = jnp.concatenate(
            [
                z_buf[pl.ds(k1, second_len, stride=double_pad), :],
                z_buf[pl.ds(pad + k1, second_len, stride=double_pad), :],
            ],
            axis=0,
        ).astype(bf16)
        spec = jnp.dot(inner[...], stacked, preferred_element_type=f32)
        re, im = spec[:second_len], spec[second_len:]
        left_re = jnp.where(low, re, lane_roll(re, chan))
        left_im = jnp.where(low, im, lane_roll(im, chan))
        right_re = jnp.where(mid, lane_roll(re, -chan), lane_roll(re, -step))
        right_im = jnp.where(mid, lane_roll(im, -chan), lane_roll(im, -step)) * sign
        corr_re = jnp.where(lane_k < step, right_re, lane_roll(re, step))
        corr_im = jnp.where(lane_k < step, right_im, lane_roll(im, step) * sign)
        out = jnp.concatenate(
            [
                left_re * corr_re - left_im * corr_im,
                left_re * corr_im + left_im * corr_re,
            ],
            axis=0,
        ).astype(bf16)
        back = jnp.dot(outer[...], out, preferred_element_type=f32)
        v_buf[pl.ds(k1, second_len, stride=double_pad), :] = back[:second_len]
        v_buf[pl.ds(pad + k1, second_len, stride=double_pad), :] = back[second_len:]
        return 0

    unroll = 3 if kept % 3 == 0 else 5 if kept % 5 == 0 else 1
    lax.fori_loop(0, kept, stage_two, 0, unroll=unroll)

    def stage_three(n2, _):
        part = v_buf[pl.ds(pl.multiple_of(n2 * double_pad, 8), double_pad), :].astype(bf16)
        at = pl.ds(n2, half, stride=second_len)
        y_out[at, :] = (
            jnp.dot(inv[n2], part, preferred_element_type=f32) + skip[...] * x_buf[at, :]
        )
        return 0

    lax.fori_loop(0, second_len, stage_three, 0, unroll=8)

    for d in range(n):
        packed = y_out[pl.ds(d * pos, rows), :]
        for j in range(1, fold):
            packed = jnp.where(
                lane >= j * step,
                lane_roll(y_out[pl.ds(d * pos + j * rows, rows), :], j * step),
                packed,
            )
        send_two[d] = packed.astype(bf16)
    for k in range(1, n):
        copy(send_two, recv_two, 1, k).start()
    recv_two[me] = send_two[me]
    for k in range(1, n):
        copy(send_two, recv_two, 1, k).wait()

    per_tile = LANES // chan
    for tile in range(width // LANES):
        for j in range(fold):
            conv_acc = jnp.zeros((rows, LANES), f32)
            grad_acc = jnp.zeros((rows, LANES), f32)
            for i in range(per_tile):
                block = recv_two[tile * per_tile + i].astype(f32)
                own = (lane >= i * chan) & (lane < (i + 1) * chan)
                conv_acc = jnp.where(own, lane_roll(block, i * chan - j * step), conv_acc)
                grad_acc = jnp.where(own, lane_roll(block, i * chan - j * step - chan), grad_acc)
            at = pl.ds(j * rows, rows)
            conv_buf[0, at, tile * LANES : (tile + 1) * LANES] = conv_acc
            conv_buf[1, at, tile * LANES : (tile + 1) * LANES] = grad_acc

    conv = conv_buf[0]
    grad_mixed = conv_buf[1]
    gated = (gates[0].astype(f32) * conv).astype(bf16)
    grad_proj = jnp.concatenate(
        [
            (gates[3].astype(f32) * conv).astype(bf16),
            (grad_mixed * gates[2].astype(f32)).astype(bf16),
            (grad_mixed * gates[1].astype(f32)).astype(bf16),
        ],
        axis=1,
    )
    first = (((0,), (0,)), ((), ()))
    grad_in = lax.dot_general(tok[...], grad_proj, first, preferred_element_type=f32) * scale
    grad_out = lax.dot_general(gated, og[...], first, preferred_element_type=f32) * scale
    at = 0
    for block in (grad_in, grad_out):
        for j in range(block.shape[1] // LANES):
            pk_out[at : at + width, :] = block[:, j * LANES : (j + 1) * LANES].astype(bf16)
            at += width
    gt_out[...] = lax.dot_general(
        grad_proj, inw[...], (((1,), (1,)), ((), ())), preferred_element_type=f32
    ).astype(bf16)


def sum_kernel(ns, nb, a_in, b_in, a_out, b_out, *scratch):
    me_s, me_b = lax.axis_index("seq"), lax.axis_index("batch")
    sems = scratch[-1]
    barrier = pltpu.get_barrier_semaphore()
    for axis, me, n in (("seq", me_s, ns), ("batch", me_b, nb)):
        for k in range(1, n):
            pl.semaphore_signal(
                barrier, inc=1, device_id={axis: lax.rem(me + k, n)}, device_id_type=MESH
            )
    pl.semaphore_wait(barrier, ns + nb - 2)

    def remote(src, dst, phase, k, which, axis, dest):
        return pltpu.make_async_remote_copy(
            src_ref=src,
            dst_ref=dst,
            send_sem=sems.at[phase, 0, k, which],
            recv_sem=sems.at[phase, 1, k, which],
            device_id={axis: dest},
            device_id_type=MESH,
        )

    streams = []
    for which, (src, out) in enumerate(((a_in, a_out), (b_in, b_out))):
        streams.append((which, src, out) + scratch[4 * which : 4 * which + 4])

    def run(make):
        for k, items in make:
            for item in items:
                item.start()
        for k, items in make:
            for item in items:
                item.wait()

    def ds(start, size, unit):
        return pl.ds(pl.multiple_of(start, unit), size)

    def unit_of(ref):
        return 16 if ref.dtype == jnp.bfloat16 else 8

    run(
        [
            (
                k,
                [
                    remote(
                        src.at[ds(lax.rem(me_b + k, nb) * got.shape[1], got.shape[1], unit_of(src))],
                        got.at[k - 1],
                        0,
                        k,
                        which,
                        "batch",
                        lax.rem(me_b + k, nb),
                    )
                    for which, src, out, got, part, got_two, whole in streams
                ],
            )
            for k in range(1, nb)
        ]
    )
    for which, src, out, got, part, got_two, whole in streams:
        size = got.shape[1]
        total = src[ds(me_b * size, size, unit_of(src)), :].astype(jnp.float32)
        for k in range(1, nb):
            total = total + got[k - 1].astype(jnp.float32)
        part[...] = total.astype(part.dtype)
    run(
        [
            (
                k,
                [
                    remote(
                        part.at[
                            ds(lax.rem(me_s + k, ns) * got_two.shape[1], got_two.shape[1], unit_of(src))
                        ],
                        got_two.at[k - 1],
                        1,
                        k,
                        which,
                        "seq",
                        lax.rem(me_s + k, ns),
                    )
                    for which, src, out, got, part, got_two, whole in streams
                ],
            )
            for k in range(1, ns)
        ]
    )
    for which, src, out, got, part, got_two, whole in streams:
        size = got_two.shape[1]
        total = part[ds(me_s * size, size, unit_of(src)), :].astype(jnp.float32)
        for k in range(1, ns):
            total = total + got_two[k - 1].astype(jnp.float32)
        whole[ds(me_b * part.shape[0] + me_s * size, size, unit_of(src)), :] = total.astype(whole.dtype)

    def spread(phase, axis, me, n, size_of):
        made = []
        for k in range(1, n):
            items = []
            for which, src, out, got, part, got_two, whole in streams:
                size = size_of(part, got_two)
                start = me_b * part.shape[0]
                if axis == "seq":
                    start = start + me_s * size
                at = whole.at[ds(start, size, unit_of(src))]
                items.append(remote(at, at, phase, k, which, axis, lax.rem(me + k, n)))
            made.append((k, items))
        run(made)

    spread(2, "seq", me_s, ns, lambda part, got_two: got_two.shape[1])
    spread(3, "batch", me_b, nb, lambda part, got_two: part.shape[0])
    for which, src, out, got, part, got_two, whole in streams:
        out[...] = whole[...]


def vmem(count):
    return [pl.BlockSpec(memory_space=pltpu.VMEM)] * count


def sine_cosine(angle):
    turns = jnp.round(angle * (1.0 / (2.0 * math.pi)))
    reduced = angle - turns * 6.28125
    reduced = reduced - turns * 0.0019350051879882812
    reduced = reduced - turns * 3.0199157663146e-07
    half = reduced * 0.5
    square = half * half
    sin = half * (
        1.0
        + square
        * (-1.0 / 6 + square * (1.0 / 120 + square * (-1.0 / 5040 + square * (1.0 / 362880 - square / 39916800.0))))
    )
    cos = 1.0 + square * (
        -0.5
        + square
        * (1.0 / 24 + square * (-1.0 / 720 + square * (1.0 / 40320 + square * (-1.0 / 3628800 + square / 479001600.0))))
    )
    return 2.0 * sin * cos, 1.0 - 2.0 * sin * sin


def embedding(positions, length, band_count):
    scaled = positions / length
    rows_list = [scaled]
    for band_index in range(1, band_count + 1):
        angle = 2.0 * math.pi * band_index * scaled
        sin, cos = sine_cosine(angle)
        rows_list.append(cos)
        rows_list.append(sin)
    return jnp.stack(rows_list, axis=0)


def contract(left, right, dims, precision=highest):
    return lax.dot_general(left, right, ((dims[:1], dims[1:]), ((), ())), precision=precision)


def shards(
    tokens,
    out_grad,
    in_weight,
    out_weight,
    skip_bias,
    embed_weight,
    embed_bias,
    hidden_weight,
    hidden_bias,
    filter_weight,
    sine_freq,
    decay_rate,
):
    f32, bf16 = jnp.float32, jnp.bfloat16
    tok, og = tokens[0], out_grad[0]
    pos, width = tok.shape
    ns, nb = lax.axis_size("seq"), lax.axis_size("batch")
    length = pos * ns
    me = lax.axis_index("seq")
    chan = width // ns
    step = 2 * chan
    start = me * chan
    hid = hidden_weight.shape[0]
    grad_scale = 1.0 / math.sqrt(nb * length)
    filter_scale = grad_scale / 4.0

    def place(part, at):
        return jnp.pad(part, ((0, 0), (at, LANES - at - chan)))

    weight_part = place(lax.dynamic_slice_in_dim(filter_weight, start, chan, 1), step)
    decay_part = lax.dynamic_slice_in_dim(decay_rate, start, chan, 0)[None]
    skip_part = lax.dynamic_slice_in_dim(skip_bias, start, chan, 0)[None]
    skip_row = place(skip_part, 0) + place(skip_part, chan)
    decay_row = place(decay_part, step)
    lane = jnp.arange(LANES)[None]
    own = (lane >= step) & (lane < step + chan)
    positions = jnp.arange(length, dtype=f32)
    modul = jnp.where(own, 4.0 * jnp.exp(-decay_row * positions[:, None]) / math.sqrt(length), 0.0)

    embed_rows = embedding(positions, length, (embed_weight.shape[0] - 1) // 2)
    pre_one = contract(embed_weight, embed_rows, (0, 0)) + embed_bias[:, None]
    act_one, cos_one = sine_cosine(sine_freq[0][:, None] * pre_one)
    pre_two = contract(hidden_weight, act_one, (0, 0)) + hidden_bias[:, None]
    act_two, cos_two = sine_cosine(sine_freq[1][:, None] * pre_two)
    filt = contract(act_two, weight_part, (0, 0)) * modul

    fwd, inv, inner, outer = make_tables(length)
    second_len, double_pad, half = fwd.shape
    fold = LANES // step
    rows = pos // fold
    main_rows = 4 * width * width // LANES
    pair = (ns, rows, LANES)
    spectral = (second_len * double_pad, LANES)
    grad_tokens, main, y, bias_part = pl.pallas_call(
        functools.partial(conv_kernel, ns, chan, grad_scale),
        out_shape=(
            jax.ShapeDtypeStruct((pos, width), bf16),
            jax.ShapeDtypeStruct((main_rows, LANES), bf16),
            jax.ShapeDtypeStruct((length, LANES), f32),
            jax.ShapeDtypeStruct((1, width), f32),
        ),
        in_specs=vmem(10),
        out_specs=tuple(vmem(4)),
        scratch_shapes=[
            pltpu.VMEM(pair, bf16),
            pltpu.VMEM(pair, bf16),
            pltpu.VMEM(pair, bf16),
            pltpu.VMEM(pair, bf16),
            pltpu.VMEM((4, pos, width), bf16),
            pltpu.VMEM((length, LANES), f32),
            pltpu.VMEM(spectral, f32),
            pltpu.VMEM(spectral, f32),
            pltpu.VMEM((2, pos, width), f32),
            pltpu.SemaphoreType.DMA((4, ns)),
        ],
        compiler_params=pltpu.CompilerParams(collective_id=0, has_side_effects=True),
        name="conv",
    )(tok, og, in_weight, out_weight, filt, skip_row, fwd, inv, inner, outer)

    high = lax.Precision.HIGH
    grad_kernel = jnp.where(own, y, 0.0) * modul
    grad_weight_part = contract(act_two, grad_kernel, (1, 0), high)
    grad_act_two = contract(weight_part, grad_kernel, (1, 1), high)
    grad_pre_two = grad_act_two * sine_freq[1][:, None] * cos_two
    grad_freq_two = jnp.sum(grad_act_two * pre_two * cos_two, axis=1)
    grad_hidden_bias = jnp.sum(grad_pre_two, axis=1)
    grad_hidden_weight = contract(act_one, grad_pre_two, (1, 1), high)
    grad_act_one = contract(hidden_weight, grad_pre_two, (1, 0), high)
    grad_pre_one = grad_act_one * sine_freq[0][:, None] * cos_one
    grad_freq_one = jnp.sum(grad_act_one * pre_one * cos_one, axis=1)
    grad_embed_bias = jnp.sum(grad_pre_one, axis=1)
    grad_embed_weight = contract(embed_rows, grad_pre_one, (1, 1), high)

    smalls = [
        grad_hidden_weight,
        grad_embed_weight,
        grad_embed_bias,
        grad_hidden_bias,
        jnp.stack([grad_freq_one, grad_freq_two], axis=0),
    ]
    flat = jnp.concatenate([s.reshape(-1) for s in smalls]) * filter_scale
    flat = jnp.concatenate([flat, bias_part[0] * grad_scale])
    flat_rows = -(-flat.shape[0] // LANES)
    flat = jnp.pad(flat, (0, flat_rows * LANES - flat.shape[0])).reshape(flat_rows, LANES)
    zero = jnp.zeros((hid, width), f32)
    grad_filter_weight = lax.dynamic_update_slice_in_dim(
        zero, grad_weight_part[:, step : step + chan] * filter_scale, start, 1
    )
    tiles = width // LANES
    blocks = [grad_filter_weight[:, j * LANES : (j + 1) * LANES] for j in range(tiles)]
    extra = jnp.concatenate(blocks + [flat], axis=0)
    unit = ns * nb * 8
    extra_rows = -(-extra.shape[0] // unit) * unit
    extra = jnp.pad(extra, ((0, extra_rows - extra.shape[0]), (0, 0)))
    unit = ns * nb * 16
    all_rows = -(-main_rows // unit) * unit
    if all_rows != main_rows:
        main = jnp.pad(main, ((0, all_rows - main_rows), (0, 0)))

    scratch = []
    for count, kind in ((all_rows, bf16), (extra_rows, f32)):
        scratch += [
            pltpu.VMEM((nb - 1, count // nb, LANES), kind),
            pltpu.VMEM((count // nb, LANES), kind),
            pltpu.VMEM((ns - 1, count // nb // ns, LANES), kind),
            pltpu.VMEM((count, LANES), kind),
        ]
    main, extra = pl.pallas_call(
        functools.partial(sum_kernel, ns, nb),
        out_shape=(
            jax.ShapeDtypeStruct((all_rows, LANES), bf16),
            jax.ShapeDtypeStruct((extra_rows, LANES), f32),
        ),
        in_specs=vmem(2),
        out_specs=tuple(vmem(2)),
        scratch_shapes=scratch + [pltpu.SemaphoreType.DMA((4, 2, max(ns, nb), 2))],
        compiler_params=pltpu.CompilerParams(collective_id=1, has_side_effects=True),
        name="sums",
    )(main, extra)

    def unpack(block, columns):
        parts = block.reshape(columns // LANES, -1, LANES)
        return jnp.concatenate([parts[j] for j in range(columns // LANES)], axis=1)

    main = main.astype(f32)
    grad_in = unpack(main[: 3 * width * tiles], 3 * width)
    grad_out = unpack(main[3 * width * tiles : main_rows], width)
    grad_filter = unpack(extra[: hid * tiles], width)
    flat = extra[hid * tiles : hid * tiles + flat_rows].reshape(-1)
    pieces, at = [], 0
    for s in smalls + [skip_bias]:
        pieces.append(flat[at : at + s.size].reshape(s.shape))
        at += s.size
    return (
        grad_tokens[None],
        grad_in,
        grad_out,
        pieces[5],
        pieces[1],
        pieces[2],
        pieces[0],
        pieces[3],
        grad_filter,
        pieces[4],
    )


def solution(mesh):
    batched = P("batch", "seq", None)
    return jax.shard_map(
        shards,
        mesh=mesh,
        in_specs=(batched, batched) + (P(),) * 10,
        out_specs=(batched,) + (P(),) * 9,
        check_vma=False,
    )
```

```python
import functools
import math

import jax
import jax.numpy as jnp
import numpy as np
from jax import lax
from jax.experimental import pallas as pl
from jax.experimental.pallas import tpu as pltpu
from jax.sharding import PartitionSpec as P

highest = lax.Precision.HIGHEST
MESH = pl.DeviceIdType.MESH
LANES = 128
VMEM_BYTES = 66 * 1000 * 1000


def factor(length):
    total = 2 * length
    first_len = 2
    while first_len * first_len < total and total % (2 * first_len) == 0:
        first_len = first_len * 2
    return first_len, total // first_len


def make_tables(length):
    total = 2 * length
    first_len, second_len = factor(length)
    half = first_len // 2
    kept = half + 1
    pad = -(-kept // 8) * 8
    k1 = np.arange(kept)[None, :, None]
    n1 = np.arange(half)[None, None, :]
    n2 = np.arange(second_len)[:, None, None]
    angle = 2.0 * np.pi * ((k1 * (n1 * second_len + n2)) % total) / total
    fwd = np.zeros((second_len, 2 * pad, half), np.float32)
    fwd[:, :kept] = np.cos(angle)
    fwd[:, pad : pad + kept] = -np.sin(angle)
    weight = np.where((k1 == 0) | (k1 == half), 1.0, 2.0) / total
    inv = np.zeros((second_len, half, 2 * pad), np.float32)
    inv[:, :, :kept] = np.swapaxes(weight * np.cos(angle), 1, 2)
    inv[:, :, pad : pad + kept] = np.swapaxes(-weight * np.sin(angle), 1, 2)
    index = np.arange(second_len)
    small = 2.0 * np.pi * ((index[:, None] * index[None, :]) % second_len) / second_len
    cos, sin = np.cos(small), np.sin(small)
    inner = np.block([[cos, sin], [-sin, cos]])
    outer = np.block([[cos, -sin], [sin, cos]])
    return tuple(jnp.asarray(t, jnp.bfloat16) for t in (fwd, inv, inner, outer))


def lane_roll(value, shift):
    shift = shift % LANES
    return value if shift == 0 else pltpu.roll(value, shift, 1)


def dot_as(left, right, dims):
    return lax.dot_general(
        left,
        right,
        ((dims[:1], dims[1:]), ((), ())),
        precision=highest,
        preferred_element_type=jnp.float32,
    )


def step_kernel(
    axis_n,
    batch_n,
    chan,
    scale,
    tok,
    og,
    inw,
    outw,
    embed,
    embed_w,
    columns,
    hidden_w,
    filter_w,
    rates,
    fwd,
    inv,
    inner,
    outer,
    gt_out,
    a_out,
    b_out,
    send_one,
    recv_one,
    send_two,
    recv_two,
    gates,
    x_buf,
    y_out,
    z_buf,
    v_buf,
    net,
    conv_buf,
    sems,
    pk_out,
    extra,
    *sum_scratch,
):
    n = axis_n
    me = lax.axis_index("seq")
    pos, width = tok.shape
    rows = send_one.shape[1]
    fold = pos // rows
    step = 2 * chan
    second_len, double_pad, half = fwd.shape
    pad = double_pad // 2
    kept = half + 1
    f32, bf16 = jnp.float32, jnp.bfloat16

    barrier = pltpu.get_barrier_semaphore()
    for axis, own_at, count in (("seq", me, n), ("batch", lax.axis_index("batch"), batch_n)):
        for k in range(1, count):
            pl.semaphore_signal(
                barrier, inc=1, device_id={axis: lax.rem(own_at + k, count)}, device_id_type=MESH
            )

    proj = jnp.dot(tok[...], inw[...], preferred_element_type=f32)
    gate_out = proj[:, :width].astype(bf16)
    gate_in = proj[:, width : 2 * width].astype(bf16)
    values = proj[:, 2 * width :].astype(bf16)
    gated_grad = lax.dot_general(
        og[...], outw[...], (((1,), (1,)), ((), ())), preferred_element_type=f32
    ).astype(bf16)
    gates[0] = gate_out
    gates[1] = gate_in
    gates[2] = values
    gates[3] = gated_grad
    mixed = (values.astype(f32) * gate_in.astype(f32)).astype(bf16).astype(f32)
    grad = (gated_grad.astype(f32) * gate_out.astype(f32)).astype(bf16).astype(f32)
    bias_sum = jnp.sum(mixed * grad, axis=0, keepdims=True) * scale

    lane = lax.broadcasted_iota(jnp.int32, (rows, LANES), 1)
    lane_full = lax.broadcasted_iota(jnp.int32, (pos, LANES), 1)
    for d in range(n):
        tile, off = (d * chan) // LANES * LANES, (d * chan) % LANES
        both = jnp.where(
            lane_full < chan,
            lane_roll(mixed[:, tile : tile + LANES], -off),
            lane_roll(grad[:, tile : tile + LANES], chan - off),
        )
        packed = both[:rows]
        for j in range(1, fold):
            packed = jnp.where(
                lane >= j * step, lane_roll(both[j * rows : (j + 1) * rows], j * step), packed
            )
        send_one[d] = packed.astype(bf16)

    pl.semaphore_wait(barrier, n + batch_n - 2)

    def copy(send, recv, which, k):
        dest = lax.rem(me + k, n)
        return pltpu.make_async_remote_copy(
            src_ref=send.at[dest],
            dst_ref=recv.at[me],
            send_sem=sems.at[2 * which, k],
            recv_sem=sems.at[2 * which + 1, k],
            device_id={"seq": dest},
            device_id_type=MESH,
        )

    for k in range(1, n):
        copy(send_one, recv_one, 0, k).start()
    recv_one[me] = send_one[me]
    v_buf[...] = jnp.zeros_like(v_buf)
    extra[...] = jnp.zeros_like(extra)
    length = x_buf.shape[0]
    hid = hidden_w.shape[0]
    tiles = width // LANES

    def select_own(value, target):
        lane_v = lax.broadcasted_iota(jnp.int32, (value.shape[0], LANES), 1)
        got = jnp.zeros((value.shape[0], LANES), f32)
        for i in range(n):
            tile, off = (i * chan) // LANES * LANES, (i * chan) % LANES
            part = lane_roll(value[:, tile : tile + LANES], target - off)
            got = jnp.where(jnp.logical_and(me == i, lane_v >= 0), part, got)
        return jnp.where((lane_v >= target) & (lane_v < target + chan), got, 0.0)

    weight = select_own(filter_w[...], step)
    rate = select_own(rates[...], step)
    skip_at = select_own(rates[...], 0) + select_own(rates[...], chan)
    decay, skip = rate[0:1], skip_at[1:2]
    freq_one, freq_two = columns[:, 0:1], columns[:, 1:2]
    tile_rows = min(256, length)

    def modulation(at_row):
        time = (lax.broadcasted_iota(jnp.int32, (tile_rows, LANES), 0) + at_row).astype(f32)
        return jnp.exp(-decay * time) * (4.0 / math.sqrt(length))

    def net_forward(i, _):
        at = pl.ds(pl.multiple_of(i * tile_rows, tile_rows), tile_rows)
        pre_one = dot_as(embed_w[...], embed[:, at], (0, 0)) + columns[:, 2:3]
        act_one, cos_one = sine_cosine(freq_one * pre_one)
        pre_two = dot_as(hidden_w[...], act_one, (0, 0)) + columns[:, 3:4]
        act_two, cos_two = sine_cosine(freq_two * pre_two)
        net[0, :, at] = pre_one
        net[1, :, at] = act_one
        net[2, :, at] = cos_one
        net[3, :, at] = pre_two
        net[4, :, at] = act_two
        net[5, :, at] = cos_two
        y_out[at, :] = dot_as(act_two, weight, (0, 0)) * modulation(i * tile_rows)
        return 0

    lax.fori_loop(0, length // tile_rows, net_forward, 0)
    for k in range(1, n):
        copy(send_one, recv_one, 0, k).wait()

    for s in range(n):
        block = recv_one[s].astype(f32)
        for j in range(fold):
            at = pl.ds(s * pos + j * rows, rows)
            x_buf[at, :] = jnp.where(lane < step, lane_roll(block, -j * step), y_out[at, :])

    def stage_one(n2, _):
        part = x_buf[pl.ds(n2, half, stride=second_len), :].astype(bf16)
        z_buf[pl.ds(pl.multiple_of(n2 * double_pad, 8), double_pad), :] = jnp.dot(
            fwd[n2], part, preferred_element_type=f32
        )
        return 0

    lax.fori_loop(0, second_len, stage_one, 0, unroll=8)

    lane_k = lax.broadcasted_iota(jnp.int32, (second_len, LANES), 1)
    low = lane_k < step
    mid = (lane_k >= chan) & (lane_k < step)
    sign = jnp.where((lane_k >= chan), -1.0, 1.0).astype(f32)

    def stage_two(k1, _):
        stacked = jnp.concatenate(
            [
                z_buf[pl.ds(k1, second_len, stride=double_pad), :],
                z_buf[pl.ds(pad + k1, second_len, stride=double_pad), :],
            ],
            axis=0,
        ).astype(bf16)
        spec = jnp.dot(inner[...], stacked, preferred_element_type=f32)
        re, im = spec[:second_len], spec[second_len:]
        left_re = jnp.where(low, re, lane_roll(re, chan))
        left_im = jnp.where(low, im, lane_roll(im, chan))
        right_re = jnp.where(mid, lane_roll(re, -chan), lane_roll(re, -step))
        right_im = jnp.where(mid, lane_roll(im, -chan), lane_roll(im, -step)) * sign
        corr_re = jnp.where(lane_k < step, right_re, lane_roll(re, step))
        corr_im = jnp.where(lane_k < step, right_im, lane_roll(im, step) * sign)
        out = jnp.concatenate(
            [
                left_re * corr_re - left_im * corr_im,
                left_re * corr_im + left_im * corr_re,
            ],
            axis=0,
        ).astype(bf16)
        back = jnp.dot(outer[...], out, preferred_element_type=f32)
        v_buf[pl.ds(k1, second_len, stride=double_pad), :] = back[:second_len]
        v_buf[pl.ds(pad + k1, second_len, stride=double_pad), :] = back[second_len:]
        return 0

    unroll = 3 if kept % 3 == 0 else 5 if kept % 5 == 0 else 1
    lax.fori_loop(0, kept, stage_two, 0, unroll=unroll)

    def stage_three(n2, _):
        part = v_buf[pl.ds(pl.multiple_of(n2 * double_pad, 8), double_pad), :].astype(bf16)
        at = pl.ds(n2, half, stride=second_len)
        y_out[at, :] = (
            jnp.dot(inv[n2], part, preferred_element_type=f32) + skip * x_buf[at, :]
        )
        return 0

    lax.fori_loop(0, second_len, stage_three, 0, unroll=8)

    for d in range(n):
        packed = y_out[pl.ds(d * pos, rows), :]
        for j in range(1, fold):
            packed = jnp.where(
                lane >= j * step,
                lane_roll(y_out[pl.ds(d * pos + j * rows, rows), :], j * step),
                packed,
            )
        send_two[d] = packed.astype(bf16)
    for k in range(1, n):
        copy(send_two, recv_two, 1, k).start()
    recv_two[me] = send_two[me]

    lane_t = lax.broadcasted_iota(jnp.int32, (tile_rows, LANES), 1)
    owned = (lane_t >= step) & (lane_t < step + chan)

    def net_backward(i, carry):
        at = pl.ds(pl.multiple_of(i * tile_rows, tile_rows), tile_rows)
        grad_kernel = jnp.where(owned, y_out[at, :], 0.0) * modulation(i * tile_rows)
        grad_weight = dot_as(net[4, :, at], grad_kernel, (1, 0))
        grad_act_two = dot_as(weight, grad_kernel, (1, 1)) * net[5, :, at]
        grad_pre_two = grad_act_two * freq_two
        grad_hidden = dot_as(net[1, :, at], grad_pre_two, (1, 1))
        grad_act_one = dot_as(hidden_w[...], grad_pre_two, (1, 0)) * net[2, :, at]
        grad_pre_one = grad_act_one * freq_one
        rows_at = embed[:, at]
        new = (
            grad_weight,
            grad_hidden,
            dot_as(rows_at, grad_pre_one, (1, 1)),
            dot_as(rows_at, grad_pre_two, (1, 1)),
            dot_as(rows_at, grad_act_one * net[0, :, at], (1, 1)),
            dot_as(rows_at, grad_act_two * net[3, :, at], (1, 1)),
        )
        return tuple(old + term for old, term in zip(carry, new))

    zeros = lambda r, c: jnp.zeros((r, c), f32)
    em = embed.shape[0]
    sums = lax.fori_loop(
        0,
        length // tile_rows,
        net_backward,
        (zeros(hid, LANES), zeros(hid, hid)) + (zeros(em, hid),) * 4,
    )
    sums = tuple(term * (scale * 0.25) for term in sums)
    lane_h = lax.broadcasted_iota(jnp.int32, (hid, LANES), 1)
    for tile in range(tiles):
        placed = zeros(hid, LANES)
        for i in range(n):
            if (i * chan) // LANES == tile:
                off = (i * chan) % LANES
                mask = (lane_h >= off) & (lane_h < off + chan) & (me == i)
                placed = jnp.where(mask, lane_roll(sums[0], off - step), placed)
        extra[tile * hid : (tile + 1) * hid, :] = placed
    base = tiles * hid
    extra[base : base + hid, 0:hid] = sums[1]
    base += hid
    for term in sums[2:]:
        extra[base : base + em, 0:hid] = term
        base += em
    for tile in range(tiles):
        extra[base + tile : base + tile + 1, :] = bias_sum[:, tile * LANES : (tile + 1) * LANES]

    main_sum = make_sum(n, batch_n, pk_out, a_out, sum_scratch[:5], 0)
    extra_sum = make_sum(n, batch_n, extra, b_out, sum_scratch[5:], 1)
    extra_sum.start(0)
    for k in range(1, n):
        copy(send_two, recv_two, 1, k).wait()

    per_tile = LANES // chan
    for tile in range(width // LANES):
        for j in range(fold):
            conv_acc = jnp.zeros((rows, LANES), f32)
            grad_acc = jnp.zeros((rows, LANES), f32)
            for i in range(per_tile):
                block = recv_two[tile * per_tile + i].astype(f32)
                own = (lane >= i * chan) & (lane < (i + 1) * chan)
                conv_acc = jnp.where(own, lane_roll(block, i * chan - j * step), conv_acc)
                grad_acc = jnp.where(own, lane_roll(block, i * chan - j * step - chan), grad_acc)
            at = pl.ds(j * rows, rows)
            conv_buf[0, at, tile * LANES : (tile + 1) * LANES] = conv_acc
            conv_buf[1, at, tile * LANES : (tile + 1) * LANES] = grad_acc

    conv = conv_buf[0]
    grad_mixed = conv_buf[1]
    gated = (gates[0].astype(f32) * conv).astype(bf16)
    grad_proj = jnp.concatenate(
        [
            (gates[3].astype(f32) * conv).astype(bf16),
            (grad_mixed * gates[2].astype(f32)).astype(bf16),
            (grad_mixed * gates[1].astype(f32)).astype(bf16),
        ],
        axis=1,
    )
    first = (((0,), (0,)), ((), ()))
    grad_in = lax.dot_general(tok[...], grad_proj, first, preferred_element_type=f32) * scale
    grad_out = lax.dot_general(gated, og[...], first, preferred_element_type=f32) * scale
    at = 0
    for block in (grad_in, grad_out):
        for j in range(block.shape[1] // LANES):
            pk_out[at : at + width, :] = block[:, j * LANES : (j + 1) * LANES].astype(bf16)
            at += width
    main_sum.start(0)
    gt_out[...] = lax.dot_general(
        grad_proj, inw[...], (((1,), (1,)), ((), ())), preferred_element_type=f32
    ).astype(bf16)
    for phase in range(4):
        for stream in (extra_sum, main_sum):
            stream.finish(phase)
            if phase < 3:
                stream.start(phase + 1)
            else:
                stream.out[...] = stream.whole[...]


class make_sum:
    def __init__(self, ns, nb, src, out, scratch, which):
        self.ns, self.nb, self.src, self.out, self.which = ns, nb, src, out, which
        self.got, self.part, self.got_two, self.whole, self.sems = scratch
        self.me_s, self.me_b = lax.axis_index("seq"), lax.axis_index("batch")
        self.unit = 16 if src.dtype == jnp.bfloat16 else 8
        self.long, self.short = self.got.shape[1], self.got_two.shape[1]

    def rows(self, start, size):
        return pl.ds(pl.multiple_of(start, self.unit), size)

    def copies(self, phase):
        axis, me, n = (
            ("seq", self.me_s, self.ns) if phase in (1, 2) else ("batch", self.me_b, self.nb)
        )
        made = []
        for k in range(1, n):
            dest = lax.rem(me + k, n)
            if phase == 0:
                src, dst = self.src.at[self.rows(dest * self.long, self.long)], self.got.at[k - 1]
            elif phase == 1:
                src = self.part.at[self.rows(dest * self.short, self.short)]
                dst = self.got_two.at[k - 1]
            else:
                start, size = self.me_b * self.long, self.long
                if phase == 2:
                    start, size = start + self.me_s * self.short, self.short
                src = dst = self.whole.at[self.rows(start, size)]
            made.append(
                pltpu.make_async_remote_copy(
                    src_ref=src,
                    dst_ref=dst,
                    send_sem=self.sems.at[phase, 0, k],
                    recv_sem=self.sems.at[phase, 1, k],
                    device_id={axis: dest},
                    device_id_type=MESH,
                )
            )
        return made

    def start(self, phase):
        for item in self.copies(phase):
            item.start()

    def finish(self, phase):
        for item in self.copies(phase):
            item.wait()
        if phase == 0:
            total = self.src[self.rows(self.me_b * self.long, self.long), :].astype(jnp.float32)
            for k in range(1, self.nb):
                total = total + self.got[k - 1].astype(jnp.float32)
            self.part[...] = total.astype(self.part.dtype)
        if phase == 1:
            total = self.part[self.rows(self.me_s * self.short, self.short), :].astype(jnp.float32)
            for k in range(1, self.ns):
                total = total + self.got_two[k - 1].astype(jnp.float32)
            start = self.me_b * self.long + self.me_s * self.short
            self.whole[self.rows(start, self.short), :] = total.astype(self.whole.dtype)


def unpack_kernel(main, extra, g_in, g_out, skip, emb, emb_b, hidden, hidden_b, filt, freq):
    width = g_out.shape[0]
    hid = hidden.shape[0]
    at = 0
    for ref in (g_in, g_out):
        for j in range(ref.shape[1] // LANES):
            ref[:, j * LANES : (j + 1) * LANES] = main[at : at + width, :].astype(jnp.float32)
            at += width
    tiles = width // LANES
    for j in range(tiles):
        filt[:, j * LANES : (j + 1) * LANES] = extra[j * hid : (j + 1) * hid, :]
    base = tiles * hid
    hidden[...] = extra[base : base + hid, 0:hid]
    base += hid
    count = emb.shape[0]
    em = -(-(count + 1) // 8) * 8
    emb[...] = extra[base : base + count, 0:hid]
    emb_b[...] = extra[base + count : base + count + 1, 0:hid]
    hidden_b[...] = extra[base + em + count : base + em + count + 1, 0:hid]
    freq[0:1, :] = extra[base + 2 * em + count : base + 2 * em + count + 1, 0:hid]
    freq[1:2, :] = extra[base + 3 * em + count : base + 3 * em + count + 1, 0:hid]
    base += 4 * em
    for j in range(tiles):
        skip[:, j * LANES : (j + 1) * LANES] = extra[base + j : base + j + 1, :]


def vmem(count):
    return [pl.BlockSpec(memory_space=pltpu.VMEM)] * count


def sine_cosine(angle):
    turns = jnp.round(angle * (1.0 / (2.0 * math.pi)))
    reduced = angle - turns * 6.28125
    reduced = reduced - turns * 0.0019350051879882812
    reduced = reduced - turns * 3.0199157663146e-07
    half = reduced * 0.5
    square = half * half
    sin = half * (
        1.0
        + square
        * (-1.0 / 6 + square * (1.0 / 120 + square * (-1.0 / 5040 + square * (1.0 / 362880 - square / 39916800.0))))
    )
    cos = 1.0 + square * (
        -0.5
        + square
        * (1.0 / 24 + square * (-1.0 / 720 + square * (1.0 / 40320 + square * (-1.0 / 3628800 + square / 479001600.0))))
    )
    return 2.0 * sin * cos, 1.0 - 2.0 * sin * sin


def embedding(length, count):
    rows = np.zeros((-(-(count + 1) // 8) * 8, length), np.float32)
    scaled = np.arange(length) / length
    rows[0] = scaled
    for band_index in range(1, (count - 1) // 2 + 1):
        rows[2 * band_index - 1] = np.cos(2.0 * np.pi * band_index * scaled)
        rows[2 * band_index] = np.sin(2.0 * np.pi * band_index * scaled)
    rows[count] = 1.0
    return jnp.asarray(rows)


def shards(
    tokens,
    out_grad,
    in_weight,
    out_weight,
    skip_bias,
    embed_weight,
    embed_bias,
    hidden_weight,
    hidden_bias,
    filter_weight,
    sine_freq,
    decay_rate,
):
    f32, bf16 = jnp.float32, jnp.bfloat16
    tok, og = tokens[0], out_grad[0]
    pos, width = tok.shape
    ns, nb = lax.axis_size("seq"), lax.axis_size("batch")
    length = pos * ns
    chan = width // ns
    hid = hidden_weight.shape[0]
    count = embed_weight.shape[0]
    embed = embedding(length, count)
    em = embed.shape[0]
    embed_w = jnp.pad(embed_weight, ((0, em - count), (0, 0)))
    columns = jnp.stack([sine_freq[0], sine_freq[1], embed_bias, hidden_bias], axis=1)
    rates = jnp.stack([decay_rate, skip_bias], axis=0)

    fwd, inv, inner, outer = make_tables(length)
    second_len, double_pad, half = fwd.shape
    rows = pos // (LANES // (2 * chan))
    tiles = width // LANES
    unit = ns * nb * 16
    main_rows = -(-4 * width * tiles // unit) * unit
    unit = ns * nb * 8
    extra_rows = -(-(tiles * hid + hid + 4 * em + tiles) // unit) * unit
    pair = (ns, rows, LANES)
    spectral = (second_len * double_pad, LANES)
    scratch = []
    for total, kind in ((main_rows, bf16), (extra_rows, f32)):
        scratch += [
            pltpu.VMEM((nb - 1, total // nb, LANES), kind),
            pltpu.VMEM((total // nb, LANES), kind),
            pltpu.VMEM((ns - 1, total // nb // ns, LANES), kind),
            pltpu.VMEM((total, LANES), kind),
            pltpu.SemaphoreType.DMA((4, 2, max(ns, nb))),
        ]
    grad_tokens, main, extra = pl.pallas_call(
        functools.partial(step_kernel, ns, nb, chan, 1.0 / math.sqrt(nb * length)),
        out_shape=(
            jax.ShapeDtypeStruct((pos, width), bf16),
            jax.ShapeDtypeStruct((main_rows, LANES), bf16),
            jax.ShapeDtypeStruct((extra_rows, LANES), f32),
        ),
        in_specs=vmem(14),
        out_specs=tuple(vmem(3)),
        scratch_shapes=[
            pltpu.VMEM(pair, bf16),
            pltpu.VMEM(pair, bf16),
            pltpu.VMEM(pair, bf16),
            pltpu.VMEM(pair, bf16),
            pltpu.VMEM((4, pos, width), bf16),
            pltpu.VMEM((length, LANES), f32),
            pltpu.VMEM((length, LANES), f32),
            pltpu.VMEM(spectral, f32),
            pltpu.VMEM(spectral, f32),
            pltpu.VMEM((6, hid, length), f32),
            pltpu.VMEM((2, pos, width), f32),
            pltpu.SemaphoreType.DMA((4, ns)),
            pltpu.VMEM((main_rows, LANES), bf16),
            pltpu.VMEM((extra_rows, LANES), f32),
        ]
        + scratch,
        compiler_params=pltpu.CompilerParams(
            collective_id=0, has_side_effects=True, vmem_limit_bytes=VMEM_BYTES
        ),
        name="step",
    )(
        tok,
        og,
        in_weight,
        out_weight,
        embed,
        embed_w,
        columns,
        hidden_weight,
        filter_weight,
        rates,
        fwd,
        inv,
        inner,
        outer,
    )

    shapes = (
        (width, 3 * width),
        (width, width),
        (1, width),
        (count, hid),
        (1, hid),
        (hid, hid),
        (1, hid),
        (hid, width),
        (2, hid),
    )
    out = pl.pallas_call(
        unpack_kernel,
        out_shape=tuple(jax.ShapeDtypeStruct(shape, f32) for shape in shapes),
        in_specs=vmem(2),
        out_specs=tuple(vmem(len(shapes))),
        name="unpack",
    )(main, extra)
    return (
        grad_tokens[None],
        out[0],
        out[1],
        out[2][0],
        out[3],
        out[4][0],
        out[5],
        out[6][0],
        out[7],
        out[8],
    )


def solution(mesh):
    batched = P("batch", "seq", None)
    return jax.shard_map(
        shards,
        mesh=mesh,
        in_specs=(batched, batched) + (P(),) * 10,
        out_specs=(batched,) + (P(),) * 9,
        check_vma=False,
    )
```
